32 devices in a mesh: grp: 2 (over x), freq: 16 (over z, y, core).
Axes of the slice: x: 2, y: 2, z: 4, core: 2. Of those that a mesh axis runs over, the one named last changes fastest.
Arguments:
- kernel: bfloat16 [2, 256, 1024, 1024], P(None, ('grp', 'freq')), parts along dimension 1, may hold values from -0.125 to 0.125
- recorded: float32 [2, 256, 1024, 128], P(None, ('grp', 'freq')), parts along dimension 1, may hold values from -8 to 8
- onset_time: int32 [2048, 128], P(('grp', 'freq')), parts along dimension 0, may hold values from 32 to 256, as said below
Outputs:
- focusing: float32 [256, 2048, 128], P(None, ('grp', 'freq')), parts along dimension 1
The draws below stay inside these ranges and needn't reach their ends.
There are 2 independent parts, one for each index of `grp`. The reference program is written for one: setup_inputs(seed, part) draws one part's arguments, and reference() takes and returns one part's arrays. A program takes and returns all parts, laid end to end along the dimension named above; each array names one. Nothing has to cross between parts.
Inputs may be any that keep to these rules, and one draw needn't show every extreme that they name: `onset_time`: onset sample of the window for each receiver and focal point.
All inputs are finite; a program needn't handle non-finite values.
Results may differ from the reference program's by a relative error of at most 0.012.
Values may be sent and summed in bfloat16 or wider, within the bound.
A program may use at most 192 MiB of HBM per device.

```python
import math
import jax
import jax.numpy as jnp
from jax import lax

SRC = 1024
REC = 1024
NF = 128
FOCAL = 128
ITERS = 2
NT = 256


def draw_recorded(key, part):
    shape = (2, NF, SRC, FOCAL)
    base = jax.random.normal(jax.random.fold_in(key, 21), shape, jnp.float32)
    column_log = jax.random.uniform(jax.random.fold_in(key, 22), (1, 1, 1, FOCAL), jnp.float32, -2.5, 1.5)
    tilt = jax.random.uniform(jax.random.fold_in(key, 23), (1, 1, 1, FOCAL), jnp.float32, -2.0, 2.0)
    source_log = jax.random.uniform(jax.random.fold_in(key, 24), (1, 1, SRC, 1), jnp.float32, -0.8, 0.8)
    freq_pos = (jnp.arange(NF, dtype=jnp.float32) / NF - 0.5).reshape(1, NF, 1, 1)
    value = base * jnp.exp(column_log + tilt * freq_pos + source_log)
    return jnp.clip(value, -8.0, 8.0).astype(jnp.float32)


def draw_onset_time(key, part):
    rows = jnp.arange(REC, dtype=jnp.int32)[:, None]
    base = NT // 8 + rows * (5 * NT // 8) // REC
    jitter = jax.random.randint(jax.random.fold_in(key, 11), (REC, FOCAL), 0, NT // 4 + 1, dtype=jnp.int32)
    column_shift = jax.random.randint(jax.random.fold_in(key, 12), (1, FOCAL), -(3 * NT // 8), NT // 2 + 1, dtype=jnp.int32)
    onset = jnp.clip(base + jitter + column_shift, NT // 8, NT).astype(jnp.int32)
    onset = onset.at[0, 0].set(NT // 8)
    onset = onset.at[REC - 1, 0].set(NT)
    return onset.astype(jnp.int32)


def shard_levels(rng, shape, split, least, largest):
    factor_of, own = 1.0, jax.random.fold_in(rng, 6)
    for dim, shards_of in split:
        draws = jnp.exp(jax.random.uniform(jax.random.fold_in(own, dim), (shards_of,), jnp.float32, least / len(split), largest / len(split)))
        factor_of = factor_of * jnp.repeat(draws, shape[dim] // shards_of).reshape([-1 if axis == dim else 1 for axis in range(len(shape))])
    return factor_of


def noise(own_key, extent, width, reach, shards=(), held_as=jnp.bfloat16):
    array = jax.random.normal(own_key, extent, jnp.float32) * width
    if len(shards) > 0:
        array = shard_levels(own_key, extent, shards, -0.22, 0.18) * array
    return jnp.clip(array, min=-reach, max=reach).astype(held_as)


def setup_inputs(seed: int = 0, part: int = 0) -> dict:
    seeds = jax.random.split(jax.random.key(seed), 4)
    part_keys = jax.random.split(jax.random.fold_in(seeds[3], part), 4)
    kernel = noise(part_keys[0], (2, NF, SRC, REC), (2 * REC) ** -0.5, 0.125, ((1, 16),))
    recorded = draw_recorded(jax.random.fold_in(jax.random.fold_in(seeds[3], part), 71), part)
    onset_time = draw_onset_time(jax.random.fold_in(jax.random.fold_in(seeds[3], part), 71), part)
    return {"kernel": kernel, "recorded": recorded, "onset_time": onset_time}


def dft_tables():
    samples = jnp.arange(2 * NF, dtype=jnp.int32)
    bins = jnp.arange(NF, dtype=jnp.int32)
    phase = (bins[:, None] * samples[None, :] % (2 * NF)).astype(jnp.float32) * (math.pi / NF)
    factor = 1.0 / math.sqrt(NF)
    return (jnp.cos(phase) * factor, jnp.sin(phase) * factor)

def reference(kernel, recorded, onset_time):
    highest = lax.Precision.HIGHEST
    cosine_table, sin_tab = dft_tables()
    samples = jnp.arange(2 * NF, dtype=jnp.int32)[:, None, None]
    keep_mask = (samples < onset_time[None]).astype(jnp.float32)
    kern_major = jnp.moveaxis(kernel, 1, 0)

    def apply_forward(model):
        flat_part = (model * keep_mask).reshape(2 * NF, -1)
        spec_real = jnp.dot(cosine_table, flat_part, precision=highest)
        spec_imag = -jnp.dot(sin_tab, flat_part, precision=highest)
        spectrum = jnp.stack([spec_real, spec_imag]).reshape(2, NF, REC, FOCAL).astype(jnp.bfloat16)

        def per_freq(pair):
            kern_slab, spectrum_block = pair
            kernel_real = kern_slab[0].astype(jnp.float32)
            kernel_imaginary = kern_slab[1].astype(jnp.float32)
            solution_real = spectrum_block[0].astype(jnp.float32)
            solution_imaginary = spectrum_block[1].astype(jnp.float32)
            y_real = jnp.dot(kernel_real, solution_real, precision=highest) - jnp.dot(kernel_imaginary, solution_imaginary, precision=highest)
            y_imag = jnp.dot(kernel_real, solution_imaginary, precision=highest) + jnp.dot(kernel_imaginary, solution_real, precision=highest)
            return jnp.stack([y_real, y_imag])
        return jnp.moveaxis(lax.map(per_freq, (kern_major, jnp.moveaxis(spectrum, 1, 0))), 0, 1)

    def apply_adjoint(resid):
        rounded = jnp.moveaxis(resid.astype(jnp.bfloat16), 1, 0)

        def per_freq(pair):
            kern_slab, data_slab = pair
            kernel_real = kern_slab[0].astype(jnp.float32)
            kernel_imaginary = kern_slab[1].astype(jnp.float32)
            update_real = data_slab[0].astype(jnp.float32)
            update_imaginary = data_slab[1].astype(jnp.float32)
            z_real = jnp.dot(kernel_real.T, update_real, precision=highest) + jnp.dot(kernel_imaginary.T, update_imaginary, precision=highest)
            z_imag = jnp.dot(kernel_real.T, update_imaginary, precision=highest) - jnp.dot(kernel_imaginary.T, update_real, precision=highest)
            return jnp.stack([z_real, z_imag]).astype(jnp.bfloat16)
        image_low = lax.optimization_barrier(jnp.moveaxis(lax.map(per_freq, (kern_major, rounded)), 0, 1))
        image = image_low.astype(jnp.float32)
        timed = jnp.dot(cosine_table.T, image[0].reshape(NF, -1), precision=highest) - jnp.dot(sin_tab.T, image[1].reshape(NF, -1), precision=highest)
        return timed.reshape(2 * NF, REC, FOCAL) * keep_mask
    beta_now = jnp.sqrt(jnp.sum(recorded * recorded))
    data_vec = recorded / beta_now
    model_raw = apply_adjoint(data_vec)
    alpha_now = jnp.sqrt(jnp.sum(model_raw * model_raw))
    model_vec = model_raw / alpha_now
    search = model_vec
    estimate = jnp.zeros_like(model_vec)
    phibar_now = beta_now
    rhobar_now = alpha_now
    for iteration in range(ITERS):
        data_raw = apply_forward(model_vec) - alpha_now * data_vec
        beta_now = jnp.sqrt(jnp.sum(data_raw * data_raw))
        data_vec = data_raw / beta_now
        model_raw = apply_adjoint(data_vec) - beta_now * model_vec
        alpha_now = jnp.sqrt(jnp.sum(model_raw * model_raw))
        model_vec = model_raw / alpha_now
        rho_now = jnp.sqrt(rhobar_now * rhobar_now + beta_now * beta_now)
        cosine = rhobar_now / rho_now
        sine_part = beta_now / rho_now
        theta_now = sine_part * alpha_now
        rhobar_now = -cosine * alpha_now
        phi_now = cosine * phibar_now
        phibar_now = sine_part * phibar_now
        estimate = estimate + phi_now / rho_now * search
        search = model_vec - theta_now / rho_now * search
    return estimate
```

```python
import math

import jax
import jax.numpy as jnp
from jax import lax
from jax.sharding import PartitionSpec as P

ITERS = 2
CHUNKS = 2


def dft_table(bins_total):
    samples = jnp.arange(2 * bins_total, dtype=jnp.int32)
    bins = jnp.arange(bins_total, dtype=jnp.int32)
    phase = (bins[:, None] * samples[None, :] % (2 * bins_total)).astype(jnp.float32) * (math.pi / bins_total)
    factor = 1.0 / math.sqrt(bins_total)
    return jnp.stack([jnp.cos(phase) * factor, -jnp.sin(phase) * factor])


def square_sum(values):
    return jnp.sum(values * values)


def make_body(mesh):
    members = mesh.shape["freq"]

    def joint(*values):
        row = jnp.zeros((128,), jnp.float32)
        for place, value in enumerate(values):
            row = row.at[place].set(value)
        spread = jnp.broadcast_to(row, (members, 128))
        got = lax.all_to_all(spread, "freq", split_axis=0, concat_axis=0, tiled=True)
        total = jnp.sum(got, axis=0)
        return [total[place] for place in range(len(values))]

    def body(kernel, recorded, onset_time):
        own_bins = kernel.shape[1]
        sources = kernel.shape[2]
        receivers = kernel.shape[3]
        rec_local, focal = onset_time.shape
        bins_total = own_bins * members
        times = 2 * bins_total
        part = own_bins // CHUNKS
        rows = 2 * part
        table = dft_table(bins_total).astype(jnp.bfloat16)
        table = table.reshape(2, members, CHUNKS, part, times)
        tables = [
            table[:, :, c].transpose(1, 0, 2, 3).reshape(members * rows, times) for c in range(CHUNKS)
        ]
        steps = lax.broadcasted_iota(jnp.int32, (rec_local, times, focal), 1)
        keep_mask = (steps < onset_time[:, None, :]).astype(jnp.float32)
        real = [kernel[0, c * part:(c + 1) * part] for c in range(CHUNKS)]
        imag = [kernel[1, c * part:(c + 1) * part] for c in range(CHUNKS)]

        def exchange(block):
            return lax.all_to_all(block, "freq", split_axis=0, concat_axis=0, tiled=True)

        def image_part(c, resid):
            low = resid.astype(jnp.bfloat16)
            turned = jnp.concatenate([low[..., focal:], -low[..., :focal]], axis=-1)
            z = jnp.einsum("hvi,hvg->hig", real[c], low, preferred_element_type=jnp.float32)
            z = z + jnp.einsum("hvi,hvg->hig", imag[c], turned, preferred_element_type=jnp.float32)
            z = z.astype(jnp.bfloat16).reshape(part, members, rec_local, 2, focal)
            z = z.transpose(1, 2, 3, 0, 4).reshape(members, rec_local, rows, focal)
            return exchange(z)

        def to_time(images):
            total = 0.0
            for c in range(CHUNKS):
                block = images[c].transpose(1, 0, 2, 3).reshape(rec_local, members * rows, focal)
                total = total + jnp.einsum(
                    "kt,rkq->rtq", tables[c], block, preferred_element_type=jnp.float32
                )
            return total * keep_mask

        def to_spectrum(field):
            low = field.astype(jnp.bfloat16)
            out = []
            for c in range(CHUNKS):
                spec = jnp.einsum("kt,rtq->rkq", tables[c], low, preferred_element_type=jnp.float32)
                spec = spec.astype(jnp.bfloat16).reshape(rec_local, members, rows, focal)
                out.append(exchange(spec.transpose(1, 0, 2, 3)))
            return out

        def forward_part(c, spec):
            spec = spec.reshape(receivers, 2, part, focal).transpose(2, 0, 1, 3)
            spec = spec.reshape(part, receivers, 2 * focal)
            turned = jnp.concatenate([-spec[..., focal:], spec[..., :focal]], axis=-1)
            y = jnp.einsum("hvi,hig->hvg", real[c], spec, preferred_element_type=jnp.float32)
            return y + jnp.einsum("hvi,hig->hvg", imag[c], turned, preferred_element_type=jnp.float32)

        data = []
        for c in range(CHUNKS):
            piece = recorded[:, c * part:(c + 1) * part]
            data.append(jnp.concatenate([piece[0], piece[1]], axis=-1))
        raw = to_time([image_part(c, data[c]) for c in range(CHUNKS)])
        sum_b, sum_z = joint(square_sum(recorded), square_sum(raw))
        beta = jnp.sqrt(sum_b)
        image_norm = jnp.sqrt(sum_z)
        alpha = image_norm / beta
        field, field_scale = raw, 1.0 / image_norm
        data_scale = 1.0 / beta
        phibar, rhobar = beta, alpha
        fields = [lax.optimization_barrier(raw.transpose(1, 0, 2))]
        search = [field_scale]
        estimate = [jnp.float32(0.0)]
        for iteration in range(ITERS):
            spectra = to_spectrum(field)
            fresh = []
            images = []
            data_squares = 0.0
            for c in range(CHUNKS):
                piece = forward_part(c, spectra[c]) * field_scale - (alpha * data_scale) * data[c]
                data_squares = data_squares + square_sum(piece)
                fresh.append(piece)
                if iteration + 1 < ITERS:
                    images.append(image_part(c, piece))
            (sum_u,) = joint(data_squares)
            beta = jnp.sqrt(sum_u)
            data, data_scale = fresh, 1.0 / beta
            rho = jnp.sqrt(rhobar * rhobar + beta * beta)
            cosine = rhobar / rho
            sine = beta / rho
            phi = cosine * phibar
            phibar = sine * phibar
            estimate = [e + phi / rho * s for e, s in zip(estimate, search)]
            if iteration + 1 == ITERS:
                break
            field = to_time(images) * data_scale - (beta * field_scale) * field
            (sum_v,) = joint(square_sum(field))
            alpha = jnp.sqrt(sum_v)
            field_scale = 1.0 / alpha
            theta = sine * alpha
            rhobar = -cosine * alpha
            fields.append(lax.optimization_barrier(field.transpose(1, 0, 2)))
            search = [-(theta / rho) * s for s in search] + [field_scale]
            estimate = estimate + [jnp.float32(0.0)]
        total = 0.0
        for e, f in zip(estimate, fields):
            total = total + e * f
        return total

    return body


def solution(mesh):
    placed = (
        P(None, ("grp", "freq"), None, None),
        P(None, ("grp", "freq"), None, None),
        P(("grp", "freq"), None),
    )
    return jax.shard_map(
        make_body(mesh), mesh=mesh, in_specs=placed, out_specs=P(None, ("grp", "freq"), None), check_vma=False
    )
```
